32 devices in a mesh: parts: 2 (over x), ctx: 8 (over z, y), grp: 2 (over core).
Axes of the slice: x: 2, y: 2, z: 4, core: 2. Of those that a mesh axis runs over, the one named last changes fastest.
Arguments:
- hidden_in: bfloat16 [4, 1024, 2048], P(('parts', 'grp'), 'ctx'), parts along dimension 0, may hold values from -6 to 6
- query_in: bfloat16 [4, 1024, 2048], P(('parts', 'grp'), 'ctx'), parts along dimension 0, may hold values from -6 to 6
- key_in: bfloat16 [4, 1024, 256], P(('parts', 'grp'), 'ctx'), parts along dimension 0, may hold values from -6 to 6
- value_in: bfloat16 [4, 1024, 256], P(('parts', 'grp'), 'ctx'), parts along dimension 0, may hold values from -6 to 6
- positions: int32 [3, 4, 1024], P(None, ('parts', 'grp'), 'ctx'), parts along dimension 1, may hold values from 0 to 1023, as said below
- segments: int32 [4, 1024], P(('parts', 'grp'), 'ctx'), parts along dimension 0, may hold values from 0 to 7, never falling along the last dimension, each value on 1 to 512 neighbouring positions
- expert_ids: int32 [4, 1024, 8], P(('parts', 'grp'), 'ctx'), parts along dimension 0, may hold values from 0 to 15, all different within a row; in each aligned block of 128 rows (0 to 127, 128 to 255, ..., all dimensions but the last counted through in order) at most 72 rows name the same one
- w_out: bfloat16 [2048, 2048], P(('ctx', 'grp')), may hold values from -0.125 to 0.125
- w_router: bfloat16 [2048, 16], replicated, may hold values from -0.03125 to 0.03125
- w_gate: bfloat16 [16, 2048, 768], P(('ctx', 'grp')), may hold values from -0.125 to 0.125
- w_up: bfloat16 [16, 2048, 768], P(('ctx', 'grp')), may hold values from -0.125 to 0.125
- w_down: bfloat16 [16, 768, 2048], P(('ctx', 'grp')), may hold values from -0.21875 to 0.21875
Outputs:
- residual: bfloat16 [4, 1024, 2048], P(('parts', 'grp'), 'ctx'), parts along dimension 0
- layer_out: bfloat16 [4, 1024, 2048], P(('parts', 'grp'), 'ctx'), parts along dimension 0
The draws below stay inside these ranges and needn't reach their ends.
There are 2 independent parts, one for each index of `parts`. The reference program is written for one: setup_inputs(seed, part) draws one part's arguments, and reference() takes and returns one part's arrays. A program takes and returns all parts, laid end to end along the dimension named above; an argument that names none is the same for every part. Nothing has to cross between parts.
Inputs may be any that keep to these rules, and one draw needn't show every extreme that they name: `positions`: t never falls along a sequence; a text token has time, row and column equal; the tokens of an image share one time and cover a grid of rows and columns. `segments`: ids never fall along a sequence; a document has at most 512 tokens and one has exactly that many. `expert_ids`: the 8 experts of a token differ; among the tokens of one device no expert is chosen more than 72 times, and on some device one expert is chosen exactly 72 times.
All inputs are finite; a program needn't handle non-finite values.
Results may differ from the reference program's by a relative error of at most 0.0055.
Values may be sent and summed in bfloat16 or wider, within the bound.
No kernel may reach another device: no remote copies, remote signals or barrier semaphores. Data moves between devices by JAX's collectives and lax.ppermute only.
A program may use at most 192 MiB of HBM per device.

```python
import math
import jax
import jax.numpy as jnp
import numpy as np
from jax import lax

D = 2048
HEADS = 16
KV_HEADS = 2
HD = 128
FF = 768
TOP = 8
TOK_DEV = 128
SEG_COUNT = 8
QW = 2048
KW = 256
LENGTH = 1024
SEQS = 2
EXPERTS = 16
CAP = 72
SEG_MOST = 512


def draw_positions(key, part):
    block_count = LENGTH // 64
    kind_key = jax.random.fold_in(key, 11)
    shift_key = jax.random.fold_in(key, 23)
    kinds = jax.random.randint(kind_key, (SEQS, block_count), 0, 4)
    columns = jnp.where(kinds == 1, 8, jnp.where(kinds == 2, 16, jnp.where(kinds == 3, 4, 64)))
    rows_grid = 64 // columns
    extent = jnp.where(kinds == 0, 64, jnp.maximum(rows_grid, columns))
    slack = LENGTH - jnp.sum(extent, axis=1)
    gap_block = jax.random.randint(shift_key, (SEQS,), 1, block_count)
    block_index = jnp.arange(block_count, dtype=jnp.int32)[None, :]
    base_pos = jnp.cumsum(extent, axis=1) - extent + jnp.where(block_index >= gap_block[:, None], slack[:, None], 0)
    offset = jnp.arange(64, dtype=jnp.int32)[None, None, :]
    image = (kinds != 0)[:, :, None]
    start_pos = base_pos[:, :, None]
    text_pos = start_pos + offset
    col_count = columns[:, :, None]
    time_pos = jnp.where(image, start_pos + 0 * offset, text_pos)
    row_pos = jnp.where(image, start_pos + offset // col_count, text_pos)
    col_pos = jnp.where(image, start_pos + offset % col_count, text_pos)
    stacked = jnp.stack([time_pos, row_pos, col_pos])
    return stacked.reshape(3, SEQS, LENGTH).astype(jnp.int32)


def steps_of(rng, shape, shards, low, high):
    def one(axis_at, blocks):
        steps = jax.random.uniform(jax.random.fold_in(jax.random.fold_in(rng, 6), axis_at), (blocks,), jnp.float32, low / len(shards), high / len(shards))
        return jnp.repeat(jnp.exp(steps), shape[axis_at] // blocks).reshape((-1,) + (1,) * (len(shape) - axis_at - 1))

    level = one(*shards[0])
    for cut in shards[1:]:
        level = level * one(*cut)
    return level


def profile(number_of, total, reach, skew):
    loads = [(1 << 20) // math.isqrt(rank ** skew) + 1 for rank in range(2, number_of + 1)]
    surplus, holding = total - reach - (number_of - 1), [1] * (number_of - 1)
    while surplus > 0:
        free = [i for i in range(number_of - 1) if holding[i] < reach]
        pool, left = sum([loads[i] for i in free]), surplus
        for i in free:
            extra = min(reach - holding[i], max(1, left * loads[i] // pool), surplus)
            holding[i] = holding[i] + extra
            surplus = surplus - extra
    return np.array([reach] + holding)


def ragged(stream_key, amount, total, limit, slope):
    if amount == 2:
        one = jax.random.randint(stream_key, (), max(1, total - limit), min(limit, total - 1) + 1)
        return jnp.stack([one, total - one])
    sizes = jnp.asarray(profile(amount, total, limit, slope), jnp.int32)
    pairs = (amount - 1) // 2
    source_of, taker = sizes[1:1 + 2 * pairs:2], sizes[2:2 + 2 * pairs:2]
    margin = jnp.minimum(source_of - 1, limit - taker)
    shifted = jax.random.randint(jax.random.fold_in(stream_key, 1), (pairs,), 0, 1 << 20) % (margin + 1)
    sizes = sizes.at[1:1 + 2 * pairs:2].set(source_of - shifted).at[2:2 + 2 * pairs:2].set(taker + shifted)
    return sizes[jax.random.permutation(jax.random.fold_in(stream_key, 2), amount)]


def shared_out(key, own, number, rows, count, top, reach, slope):
    order = jax.random.permutation(key, count)
    heavy_load, common = load_shares(count, rows * top, reach, slope, True), load_shares(count, rows * top, reach, slope, False)
    places = jnp.arange(count)

    def named(sizes, rotation):
        used = int((sizes > 0).sum())
        fixed = max(1, used // 4)
        shifted = fixed + (places - fixed + rotation * (used - fixed)) % max(1, count - fixed)
        return jnp.zeros((count,), jnp.int32).at[order[jnp.where(places < fixed, places, shifted)]].set(jnp.asarray(sizes, jnp.int32))

    sizes = jnp.where(number % 4 == 0, named(heavy_load, number // 4), named(common, number - number // 4 - 1))
    mixed = jax.random.permutation(jax.random.fold_in(own, 3), count)
    source_of, receiver = mixed[0:count // 2 * 2:2], mixed[1:count // 2 * 2:2]
    room = jnp.minimum(sizes[source_of] - 1, reach - sizes[receiver]) // 2
    room = jnp.where((source_of == order[0]) | (receiver == order[0]) | (sizes[receiver] == 0), 0, jnp.maximum(room, 0))
    shifted = jax.random.randint(jax.random.fold_in(own, 4), (count // 2,), 0, 1 << 20) % (room + 1)
    sizes = sizes.at[source_of].add(-shifted).at[receiver].add(shifted)
    items = jnp.searchsorted(jnp.cumsum(sizes), jnp.arange(rows * top), side="right").astype(jnp.int32)
    listing = items.reshape(top, rows).T
    listing = listing[jax.random.permutation(jax.random.fold_in(own, 1), rows)]
    rotation = jax.random.randint(jax.random.fold_in(own, 2), (rows, 1), 0, top)
    return jnp.take_along_axis(listing, (jnp.arange(top)[None, :] + rotation) % top, axis=1)


def load_shares(number_of, total, bound, skew, full):
    loads = [(1 << 20) // math.isqrt(standing ** skew) + 1 for standing in range(1, number_of + 1)]
    largest = bound if full else min(bound, max(-(-total // number_of), total * loads[0] // sum(loads)))
    least = 1 if total - largest >= number_of - 1 else 0
    holding, spare = [largest] + [least] * (number_of - 1), total - largest - least * (number_of - 1)
    while spare > 0:
        free = [i for i in range(1, number_of) if holding[i] < largest] or [i for i in range(1, number_of) if holding[i] < bound]
        mass, remaining = sum([loads[i] for i in free]), spare
        for i in free:
            more = min(bound - holding[i], max(1, remaining * loads[i] // mass), spare)
            holding[i] = holding[i] + more
            spare = spare - more
    return np.array(holding)


def noise(key, dims, deviation, reach, cuts=(), held_as=jnp.bfloat16):
    level = steps_of(key, dims, cuts, -0.22, 0.18) if cuts else 1.0
    array = jax.random.normal(key, dims, jnp.float32) * deviation * level
    return jnp.minimum(jnp.maximum(array, -reach), reach).astype(held_as)


def setup_inputs(seed: int = 0, part: int = 0) -> dict:
    arg_keys = jax.random.split(jax.random.key(seed), 13)
    part_splits = jax.random.split(jax.random.fold_in(arg_keys[12], part), 13)
    hidden_in = noise(part_splits[0], (SEQS, LENGTH, D), 1.0, 6.0, ((0, 2), (1, 8)))
    query_in = noise(part_splits[1], (SEQS, LENGTH, QW), 1.0, 6.0, ((0, 2), (1, 8)))
    key_in = noise(part_splits[2], (SEQS, LENGTH, KW), 1.0, 6.0, ((0, 2), (1, 8)))
    value_in = noise(part_splits[3], (SEQS, LENGTH, KW), 1.0, 6.0, ((0, 2), (1, 8)))
    positions = draw_positions(jax.random.fold_in(jax.random.fold_in(arg_keys[12], part), 71), part)
    segments = jax.vmap(lambda own: jnp.searchsorted(jnp.cumsum(ragged(own, SEG_COUNT, LENGTH, SEG_MOST, 1)), jnp.arange(LENGTH), side="right"))(jax.random.split(part_splits[5], SEQS)).reshape((SEQS, LENGTH)).astype(jnp.int32)
    expert_ids_keys = jax.random.split(jax.random.fold_in(part_splits[6], 1), SEQS * LENGTH // TOK_DEV)
    expert_ids_turns = jax.random.permutation(jax.random.fold_in(part_splits[6], 3), SEQS * LENGTH // TOK_DEV)
    expert_ids = jax.vmap(lambda own, number: shared_out(jax.random.fold_in(part_splits[6], 2), own, number, TOK_DEV, EXPERTS, TOP, CAP, 1))(expert_ids_keys, expert_ids_turns).reshape((SEQS, LENGTH, TOP))
    w_out = noise(arg_keys[7], (QW, D), QW ** -0.5, 0.125, ((0, 16),))
    w_router = noise(arg_keys[8], (D, EXPERTS), (16 * D) ** -0.5, 0.03125)
    w_gate = noise(arg_keys[9], (EXPERTS, D, FF), D ** -0.5, 0.125, ((0, 16),))
    w_up = noise(arg_keys[10], (EXPERTS, D, FF), D ** -0.5, 0.125, ((0, 16),))
    w_down = noise(arg_keys[11], (EXPERTS, FF, D), FF ** -0.5, 0.21875, ((0, 16),))
    return {"hidden_in": hidden_in, "query_in": query_in, "key_in": key_in, "value_in": value_in, "positions": positions, "segments": segments, "expert_ids": expert_ids, "w_out": w_out, "w_router": w_router, "w_gate": w_gate, "w_up": w_up, "w_down": w_down}


rope_base = 5000000.0
norm_eps = 1e-06

def row_norm(values):
    return values * lax.rsqrt(lax.optimization_barrier(jnp.mean(values * values, axis=-1, keepdims=True)) + norm_eps)

def rope_angles(places):
    half_size = HD // 2
    freq_index = jnp.arange(half_size, dtype=jnp.int32)
    inverse = jnp.exp(freq_index.astype(jnp.float32) * (-2.0 * math.log(rope_base) / HD))
    freq_table = np.arange(half_size)
    component = np.where(freq_table < half_size - 4, freq_table % 3, 0)
    picked = places[component, :]
    return jnp.transpose(picked).astype(jnp.float32) * inverse[None, :]

def rotate(head_rows, angles):
    half_size = HD // 2
    cosine = jnp.cos(angles)[:, None, :]
    sine_part = jnp.sin(angles)[:, None, :]
    first_half = head_rows[..., :half_size]
    second_half = head_rows[..., half_size:]
    return jnp.concatenate([first_half * cosine - second_half * sine_part, second_half * cosine + first_half * sine_part], axis=-1)

def prepare(raw_rows, head_count, angles):
    length = raw_rows.shape[0]
    head_rows = raw_rows.astype(jnp.float32).reshape(length, head_count, HD)
    return rotate(row_norm(head_rows), angles).astype(jnp.bfloat16).reshape(length, head_count * HD)

def route_gates(logits, flat_ids):
    matches = flat_ids[:, :, None] == jnp.arange(logits.shape[1], dtype=jnp.int32)[None, None, :]
    picked = lax.optimization_barrier(jnp.sum(jnp.where(matches, logits[:, None, :], 0.0), axis=-1))
    raised = jnp.exp(picked)
    return raised / lax.optimization_barrier(jnp.sum(raised, axis=-1, keepdims=True))

def expert_mlp(rows_in, gate_mat, up_mat, down_mat):
    gate_part = jnp.dot(rows_in, gate_mat, preferred_element_type=jnp.float32)
    up_part = jnp.dot(rows_in, up_mat, preferred_element_type=jnp.float32)
    acts = (jax.nn.silu(gate_part) * up_part).astype(jnp.bfloat16)
    return jnp.dot(acts, down_mat, preferred_element_type=jnp.float32).astype(jnp.bfloat16)

def reference(hidden_in, query_in, key_in, value_in, positions, segments, expert_ids, w_out, w_router, w_gate, w_up, w_down):
    length = hidden_in.shape[1]
    group_size = HEADS // KV_HEADS
    block_count = max(1, length // 512)
    block_rows = length // block_count
    score_scale = 1.0 / math.sqrt(HD)
    residual_list = []
    for sequence in range(SEQS):
        angles = rope_angles(positions[:, sequence, :])
        query_rot = prepare(query_in[sequence], HEADS, angles).reshape(length, KV_HEADS, group_size, HD)
        key_rot = prepare(key_in[sequence], KV_HEADS, angles).reshape(length, KV_HEADS, HD).astype(jnp.float32)
        value_all = value_in[sequence].reshape(length, KV_HEADS, HD).astype(jnp.float32)
        seq_ids = segments[sequence]
        key_pos = jnp.arange(length, dtype=jnp.int32)

        def attend_block(block_index):
            first_row = (block_index * block_rows).astype(jnp.int32)
            query_part = lax.dynamic_slice_in_dim(query_rot, first_row, block_rows, 0).astype(jnp.float32)
            query_pos = first_row + jnp.arange(block_rows, dtype=jnp.int32)
            query_seg = lax.dynamic_slice_in_dim(seq_ids, first_row, block_rows, 0)
            scores = jnp.einsum('qhgd,khd->hgqk', query_part, key_rot, precision=lax.Precision.HIGHEST) * score_scale
            allowed = (key_pos[None, :] <= query_pos[:, None]) & (seq_ids[None, :] == query_seg[:, None])
            weights = jnp.where(allowed[None, None], jnp.exp(scores), 0.0)
            weighted = jnp.einsum('hgqk,khd->qhgd', weights.astype(jnp.bfloat16).astype(jnp.float32), value_all, precision=lax.Precision.HIGHEST)
            totals = jnp.transpose(lax.optimization_barrier(jnp.sum(weights, axis=-1)), (2, 0, 1))
            return (weighted / totals[..., None]).astype(jnp.bfloat16).reshape(block_rows, HEADS * HD)
        attention = lax.map(attend_block, jnp.arange(block_count, dtype=jnp.int32)).reshape(length, HEADS * HD)
        projected = jnp.dot(attention, w_out, preferred_element_type=jnp.float32)
        residual_list.append((hidden_in[sequence].astype(jnp.float32) + projected).astype(jnp.bfloat16))
    residual = jnp.stack(residual_list)
    flat_rows = residual.reshape(-1, D)
    total_rows = flat_rows.shape[0]
    normed = row_norm(flat_rows.astype(jnp.float32)).astype(jnp.bfloat16)
    logits = jnp.dot(normed, w_router, preferred_element_type=jnp.float32)
    flat_ids = expert_ids.reshape(-1, TOP)
    gates = route_gates(logits, flat_ids)
    slot_total = EXPERTS * CAP

    def serve(combined, inputs):
        expert, gate_mat, up_mat, down_mat = inputs
        chosen = flat_ids == expert
        routed = jnp.any(chosen, axis=-1)
        weight_sum = lax.optimization_barrier(jnp.sum(jnp.where(chosen, gates, 0.0), axis=-1))
        slot_rank = jnp.cumsum(routed.astype(jnp.int32)) - 1
        slot_place = jnp.where(routed, slot_rank, slot_total).astype(jnp.int32)
        row_order = jnp.zeros((slot_total,), jnp.int32).at[slot_place].set(jnp.arange(total_rows, dtype=jnp.int32), mode='drop')
        filled = jnp.sum(routed.astype(jnp.int32))
        produced = expert_mlp(normed[row_order], gate_mat, up_mat, down_mat)
        target = jnp.where(jnp.arange(slot_total, dtype=jnp.int32) < filled, row_order, total_rows).astype(jnp.int32)
        combined = combined.at[target].add(weight_sum[row_order][:, None] * produced.astype(jnp.float32), mode='drop')
        return (combined, None)
    combined, unused = lax.scan(serve, jnp.zeros((total_rows, D), jnp.float32), (jnp.arange(EXPERTS, dtype=jnp.int32), w_gate, w_up, w_down))
    layer_out = (flat_rows.astype(jnp.float32) + combined).astype(jnp.bfloat16).reshape(residual.shape)
    return (residual, layer_out)
```

```python
import functools
import math

import jax
import jax.numpy as jnp
import numpy as np
from jax import lax
from jax.experimental import pallas as pl
from jax.experimental.pallas import tpu as pltpu
from jax.sharding import PartitionSpec as P

HD = 128
LANES = 128
rope_base = 5000000.0
norm_eps = 1e-06


SWAP = [(0, 1), (1, 0)]
VMEM_LIMIT = 60 * 1024 * 1024


def ring_order(count):
    return list(range(0, count, 2)) + list(range(count - 1 - count % 2, 0, -2))


def hop(value, order, step):
    count = len(order)
    return lax.ppermute(value, "ctx", [(order[i], order[(i + step) % count]) for i in range(count)])


def rope_tables(places):
    half_size = HD // 2
    freq_index = jnp.arange(half_size, dtype=jnp.int32)
    inverse = jnp.exp(freq_index.astype(jnp.float32) * (-2.0 * math.log(rope_base) / HD))
    freq_table = np.arange(half_size)
    component = np.where(freq_table < half_size - 4, freq_table % 3, 0)
    placed = places.astype(jnp.float32)
    picked = sum(
        placed[c][:, None] * jnp.asarray(component == c, jnp.float32)[None, :] for c in range(3)
    )
    angles = picked * inverse[None, :]
    cosine, sine_part = jnp.cos(angles), jnp.sin(angles)
    return (
        jnp.concatenate([cosine, cosine], axis=-1),
        jnp.concatenate([-sine_part, sine_part], axis=-1),
    )


def norm_rotate(head, cosine, sine_part):
    scaled = head * lax.rsqrt(jnp.mean(head * head, axis=-1, keepdims=True) + norm_eps)
    return scaled * cosine + pltpu.roll(scaled, HD // 2, 1) * sine_part


def key_kernel(key_ref, value_ref, cos_ref, sin_ref, seg_ref, out_ref):
    tokens, width = key_ref.shape
    for start in range(0, width, HD):
        head = key_ref[:, start : start + HD].astype(jnp.float32)
        out_ref[:tokens, start : start + HD] = norm_rotate(head, cos_ref[...], sin_ref[...]).astype(
            jnp.bfloat16
        )
    out_ref[:tokens, width:] = value_ref[...]
    numbers = (seg_ref[...] + 1).astype(jnp.float32).astype(jnp.bfloat16)
    out_ref[tokens:, :] = jnp.zeros((8, 2 * width), jnp.bfloat16)
    out_ref[tokens:, :tokens] = jnp.broadcast_to(numbers, (8, tokens))


def attention_kernel(heads_at_once, core_ref, query_ref, cos_ref, sin_ref, seg_ref, *rest):
    kv_refs, (same_ref, other_ref) = rest[:-2], rest[-2:]
    tokens = query_ref.shape[0]
    width = kv_refs[0].shape[1] // 2
    kv_heads = width // HD
    pairs = query_ref.shape[1] // HD // 2
    pairs_per_kv = pairs // kv_heads
    core = core_ref[0]
    query_seg = (seg_ref[...] + 1).astype(jnp.float32)
    masks = []
    for place, ref in enumerate(kv_refs):
        key_seg = ref[tokens : tokens + 1, :tokens].astype(jnp.float32)
        allowed = query_seg == key_seg
        if place == 0:
            row = lax.broadcasted_iota(jnp.int32, (tokens, tokens), 0)
            column = lax.broadcasted_iota(jnp.int32, (tokens, tokens), 1)
            allowed = allowed & (column <= row)
        masks.append(jnp.where(allowed, 1.0, 0.0))
    mask = jnp.concatenate(masks, axis=1)
    mask = jnp.concatenate([mask] * heads_at_once, axis=0) > 0.5
    for kv_head in range(kv_heads):
        at = kv_head * HD
        keys = jnp.concatenate([ref[:tokens, at : at + HD] for ref in kv_refs], axis=0)
        values = jnp.concatenate(
            [ref[:tokens, width + at : width + at + HD] for ref in kv_refs], axis=0
        )
        for out_ref, parity in ((other_ref, 1 - core), (same_ref, core)):
            for first in range(kv_head * pairs_per_kv, (kv_head + 1) * pairs_per_kv, heads_at_once):
                queries = []
                for pair in range(first, first + heads_at_once):
                    start = pl.multiple_of((2 * pair + parity) * HD, HD)
                    head = query_ref[:, pl.ds(start, HD)].astype(jnp.float32)
                    queries.append(
                        norm_rotate(head, cos_ref[...], sin_ref[...]).astype(jnp.bfloat16)
                    )
                scores = lax.dot_general(
                    jnp.concatenate(queries, axis=0),
                    keys,
                    (((1,), (1,)), ((), ())),
                    preferred_element_type=jnp.float32,
                ) * (1.0 / math.sqrt(HD))
                weights = jnp.where(mask, jnp.exp(scores), 0.0)
                totals = jnp.sum(weights, axis=-1, keepdims=True)
                weighted = jnp.dot(
                    weights.astype(jnp.bfloat16), values, preferred_element_type=jnp.float32
                )
                result = (weighted / totals).astype(jnp.bfloat16)
                for i in range(heads_at_once):
                    pair = first + i
                    out_ref[:, pair * HD : (pair + 1) * HD] = result[i * tokens : (i + 1) * tokens]


def project_kernel(source_ref, own_ref, partner_ref, *rest):
    chunk_refs, (own_out, partner_out) = rest[:-2], rest[-2:]
    rows = chunk_refs[0].shape[0]
    half = own_out.shape[1] // 2
    full, halves = chunk_refs[:-2], chunk_refs[-2:]
    for att_ref, out_ref in ((partner_ref, partner_out), (own_ref, own_out)):
        def part(place):
            start = pl.multiple_of(source_ref[place] * rows, rows)
            return att_ref[:, pl.ds(start, rows)]

        attended = jnp.concatenate([part(i) for i in range(len(full) + 1)], axis=1)
        for side in range(2):
            columns = slice(side * half, (side + 1) * half)
            weights = jnp.concatenate(
                [ref[:, columns] for ref in full] + [halves[side][...]], axis=0
            )
            out_ref[:, columns] = jnp.dot(attended, weights, preferred_element_type=jnp.float32)


def norm_kernel(experts, hidden_ref, own_ref, other_ref, router_ref, ids_ref, residual_ref, out_ref):
    tokens, width = hidden_ref.shape
    residual = (hidden_ref[...].astype(jnp.float32) + (own_ref[...] + other_ref[...])).astype(
        jnp.bfloat16
    )
    residual_ref[...] = residual
    wide = residual.astype(jnp.float32)
    normed = (
        wide * lax.rsqrt(jnp.mean(wide * wide, axis=-1, keepdims=True) + norm_eps)
    ).astype(jnp.bfloat16)
    out_ref[:, :width] = normed
    logits = jnp.dot(normed, router_ref[...], preferred_element_type=jnp.float32)
    lane = lax.broadcasted_iota(jnp.int32, logits.shape, 1)
    expert = jnp.where(lane >= experts, lane - experts, lane)
    chosen = lane < 0
    for k in range(ids_ref.shape[1]):
        chosen = chosen | (ids_ref[:, k : k + 1] == expert)
    raised = jnp.where(chosen & (lane < 2 * experts), jnp.exp(logits), 0.0)
    gates = raised / jnp.sum(jnp.where(lane < experts, raised, 0.0), axis=-1, keepdims=True)
    high = gates.astype(jnp.bfloat16)
    low = (gates - high.astype(jnp.float32)).astype(jnp.bfloat16)
    out_ref[:, width:] = jnp.where(lane < experts, high.astype(jnp.float32), low.astype(jnp.float32)).astype(
        jnp.bfloat16
    )


def expert_kernel(experts, count, expert_ref, *refs):
    x_refs = refs[:count]
    own, partner = refs[count : count + 3], refs[count + 3 : count + 6]
    out_refs = refs[count + 6 : count + 6 + count]
    x_all, gate_all, total = refs[count + 6 + count :]
    which, tile = pl.program_id(0), pl.program_id(1)
    width = x_all.shape[1]

    @pl.when((which == 0) & (tile == 0))
    def _():
        at = 0
        for ref in x_refs:
            rows = ref.shape[0]
            x_all[at : at + rows, :] = ref[:, :width]
            listed = ref[:, width:].astype(jnp.float32)
            lane = lax.broadcasted_iota(jnp.int32, listed.shape, 1)
            for i in range(2):
                number = expert_ref[i]
                picked = jnp.where((lane == number) | (lane == number + experts), listed, 0.0)
                gate_all[i, at : at + rows, :] = jnp.broadcast_to(
                    jnp.sum(picked, axis=-1, keepdims=True), (rows, LANES)
                )
            at += rows

    def serve(gate_ref, up_ref, down_ref):
        rows_in = x_all[...]
        gate_part = jnp.dot(rows_in, gate_ref[...], preferred_element_type=jnp.float32)
        up_part = jnp.dot(rows_in, up_ref[...], preferred_element_type=jnp.float32)
        acts = (gate_part / (1.0 + jnp.exp(-gate_part)) * up_part).astype(jnp.bfloat16)
        product = jnp.dot(acts, down_ref[...], preferred_element_type=jnp.float32)

        @pl.when(tile == 0)
        def _():
            total[...] = product

        @pl.when(tile > 0)
        def _():
            total[...] += product

    @pl.when(which == 0)
    def _():
        serve(*own)

    @pl.when(which == 1)
    def _():
        serve(*partner)

    @pl.when(tile == pl.num_programs(1) - 1)
    def _():
        at = 0
        for ref in out_refs:
            rows = ref.shape[0]
            gate = gate_all[which, at : at + rows, :1]
            value = gate * total[at : at + rows, :].astype(jnp.bfloat16).astype(jnp.float32)

            @pl.when(which == 0)
            def _(ref=ref, value=value):
                ref[...] = value

            @pl.when(which == 1)
            def _(ref=ref, value=value):
                ref[...] += value

            at += rows


def run_experts(blocks, expert_pair, own, partner, experts):
    width, hidden = own[0].shape
    tile = 256 if hidden % 256 == 0 else hidden
    tiles = hidden // tile
    rows = sum(block.shape[0] for block in blocks)
    count = len(blocks)

    def whole(shape):
        return pl.BlockSpec(shape, lambda e, f: (0, 0))

    def own_at(e, f):
        return jnp.where(e == 0, f, tiles - 1)

    def partner_at(e, f):
        return jnp.where(e == 0, 0, f)

    weight_specs = []
    for at in (own_at, partner_at):
        weight_specs += [
            pl.BlockSpec((width, tile), lambda e, f, at=at: (0, at(e, f))),
            pl.BlockSpec((width, tile), lambda e, f, at=at: (0, at(e, f))),
            pl.BlockSpec((tile, width), lambda e, f, at=at: (at(e, f), 0)),
        ]
    return pl.pallas_call(
        functools.partial(expert_kernel, experts, count),
        grid=(2, tiles),
        out_shape=[jax.ShapeDtypeStruct((b.shape[0], width), jnp.float32) for b in blocks],
        in_specs=[pl.BlockSpec(memory_space=pltpu.SMEM)]
        + [whole(b.shape) for b in blocks]
        + weight_specs,
        out_specs=[whole((b.shape[0], width)) for b in blocks],
        scratch_shapes=[
            pltpu.VMEM((rows, width), jnp.bfloat16),
            pltpu.VMEM((2, rows, LANES), jnp.float32),
            pltpu.VMEM((rows, width), jnp.float32),
        ],
        compiler_params=pltpu.CompilerParams(
            dimension_semantics=("arbitrary", "arbitrary"), vmem_limit_bytes=VMEM_LIMIT
        ),
        cost_estimate=pl.CostEstimate(
            flops=2 * 2 * 3 * rows * width * hidden,
            bytes_accessed=2 * 3 * width * hidden * 2 + rows * width * 6,
            transcendentals=2 * rows * hidden,
        ),
        name="experts",
    )(expert_pair, *blocks, *own, *partner)


def call(kernel, out_shape, operands, scalars=1, flops=0, name=None):
    specs = [pl.BlockSpec(memory_space=pltpu.SMEM)] * scalars
    specs += [pl.BlockSpec(memory_space=pltpu.VMEM)] * (len(operands) - scalars)
    out_specs = jax.tree.map(lambda _: pl.BlockSpec(memory_space=pltpu.VMEM), out_shape)
    moved = sum(o.size * o.dtype.itemsize for o in operands)
    return pl.pallas_call(
        kernel,
        out_shape=out_shape,
        in_specs=specs,
        out_specs=out_specs,
        compiler_params=pltpu.CompilerParams(vmem_limit_bytes=VMEM_LIMIT),
        cost_estimate=pl.CostEstimate(flops=flops, bytes_accessed=moved, transcendentals=0),
        name=name,
    )(*operands)


def ring_gather(own, order, split_axis):
    reach = len(order) // 2
    from_left, from_right = [own], [own]
    for _ in range(reach - 1):
        from_left.append(hop(from_left[-1], order, 1))
        from_right.append(hop(from_right[-1], order, -1))
    size = own.shape[split_axis] // 2
    first = lax.slice_in_dim(from_left[-1], 0, size, axis=split_axis)
    second = lax.slice_in_dim(from_right[-1], size, 2 * size, axis=split_axis)
    return from_left[1:], from_right[1:], (hop(first, order, 1), hop(second, order, -1))


def on_device(
    order,
    hidden_in,
    query_in,
    key_in,
    value_in,
    positions,
    segments,
    expert_ids,
    w_out,
    w_router,
    w_gate,
    w_up,
    w_down,
):
    tokens, width = hidden_in.shape[1:]
    count = len(order)
    reach = count // 2
    ctx, grp = lax.axis_index("ctx"), lax.axis_index("grp")
    experts = w_router.shape[1]
    key_width = key_in.shape[2]
    out_rows = w_out.shape[0]
    core = jnp.reshape(grp, (1,)).astype(jnp.int32)

    own_experts = (w_gate[0], w_up[0], w_down[0])
    partner_experts = tuple(lax.ppermute(w, "grp", SWAP) for w in own_experts)
    expert_pair = jnp.stack([2 * ctx + grp, 2 * ctx + 1 - grp]).astype(jnp.int32)

    cosine, sine_part = rope_tables(positions[:, 0, :])
    kv_own = call(
        key_kernel,
        jax.ShapeDtypeStruct((tokens + 8, 2 * key_width), jnp.bfloat16),
        (key_in[0], value_in[0], cosine, sine_part, segments),
        scalars=0,
        flops=tokens * key_width * 16,
        name="keys",
    )
    kv_blocks = [kv_own] + [
        lax.ppermute(kv_own, "ctx", [(i, i + s) for i in range(count - s)])
        for s in range(1, reach + 1)
    ]
    half_heads = jax.ShapeDtypeStruct((tokens, width // 2), jnp.bfloat16)
    same, other = call(
        functools.partial(attention_kernel, 4),
        (half_heads, half_heads),
        (core, query_in[0], cosine, sine_part, segments.reshape(tokens, 1), *kv_blocks),
        flops=4 * tokens * width * tokens * (reach + 1),
        name="attend",
    )
    aligned = out_rows % LANES == 0
    if aligned:
        from_left, from_right, farthest = ring_gather(w_out, order, 1)
        place_of = np.argsort(np.array(order))
        offsets = [0] + [-s for s in range(1, reach)] + [s for s in range(1, reach)] + [reach]
        table = np.array(
            [[order[(place_of[c] + o) % count] for o in offsets] for c in range(count)], np.int32
        )
        sources = lax.dynamic_index_in_dim(jnp.asarray(table), ctx, 0, keepdims=False)
        partner_same = lax.ppermute(other, "grp", SWAP)
        summed = jax.ShapeDtypeStruct((tokens, width), jnp.float32)
        own_part, partner_part = call(
            project_kernel,
            (summed, summed),
            (sources, same, partner_same, w_out, *from_left, *from_right, *farthest),
            flops=4 * tokens * width * width // 2,
            name="project",
        )
        other_part = lax.ppermute(partner_part, "grp", SWAP)
    else:
        heads = width // HD // 2
        stacked = jnp.stack([same.reshape(tokens, heads, HD), other.reshape(tokens, heads, HD)], axis=2)
        swapped = jnp.where(grp == 0, stacked, stacked[:, :, ::-1])
        attention = swapped.reshape(tokens, width)
        gathered = lax.all_gather(w_out, ("ctx", "grp"), axis=0, tiled=True)
        own_part = jnp.dot(attention, gathered, preferred_element_type=jnp.float32)
        other_part = jnp.zeros_like(own_part)

    side = -(-2 * experts // LANES) * LANES
    router = jnp.concatenate(
        [w_router, w_router, jnp.zeros((width, side - 2 * experts), w_router.dtype)], axis=1
    )
    residual, own_block = call(
        functools.partial(norm_kernel, experts),
        (
            jax.ShapeDtypeStruct((tokens, width), jnp.bfloat16),
            jax.ShapeDtypeStruct((tokens, width + side), jnp.bfloat16),
        ),
        (hidden_in[0], own_part, other_part, router, expert_ids[0]),
        scalars=0,
        flops=2 * tokens * width * side,
        name="norm",
    )

    serve = functools.partial(
        run_experts, expert_pair=expert_pair, own=own_experts, partner=partner_experts, experts=experts
    )
    from_left, from_right, farthest = ring_gather(own_block, order, 0)
    (own_sum,) = serve([own_block])
    sums = [serve([a, b]) for a, b in zip(from_left, from_right)]
    first, second = serve(list(farthest))

    def narrow(value):
        return value.astype(jnp.bfloat16)

    half = tokens // 2
    to_right, to_left = hop(narrow(first), order, -1), hop(narrow(second), order, 1)
    left_sum, right_sum = sums[-1]
    moving_left = narrow(
        jnp.concatenate([left_sum[:half] + to_right.astype(jnp.float32), left_sum[half:]], axis=0)
    )
    moving_right = narrow(
        jnp.concatenate([right_sum[:half], right_sum[half:] + to_left.astype(jnp.float32)], axis=0)
    )
    for place in range(reach - 3, -1, -1):
        moving_left, moving_right = hop(moving_left, order, -1), hop(moving_right, order, 1)
        left_sum, right_sum = sums[place]
        moving_left = narrow(moving_left.astype(jnp.float32) + left_sum)
        moving_right = narrow(moving_right.astype(jnp.float32) + right_sum)
    moving_left, moving_right = hop(moving_left, order, -1), hop(moving_right, order, 1)
    layer_out = narrow(
        residual.astype(jnp.float32)
        + (own_sum + (moving_left.astype(jnp.float32) + moving_right.astype(jnp.float32)))
    )
    return (residual[None], layer_out[None])


def solution(mesh):
    placed = (
        P(("parts", "grp"), "ctx", None),
        P(("parts", "grp"), "ctx", None),
        P(("parts", "grp"), "ctx", None),
        P(("parts", "grp"), "ctx", None),
        P(None, ("parts", "grp"), "ctx"),
        P(("parts", "grp"), "ctx"),
        P(("parts", "grp"), "ctx", None),
        P(("ctx", "grp"), None),
        P(),
        P(("ctx", "grp"), None, None),
        P(("ctx", "grp"), None, None),
        P(("ctx", "grp"), None, None),
    )
    return jax.shard_map(
        functools.partial(on_device, ring_order(mesh.shape["ctx"])),
        mesh=mesh,
        in_specs=placed,
        out_specs=(P(("parts", "grp"), "ctx", None), P(("parts", "grp"), "ctx", None)),
        check_vma=False,
    )
```
